128 devices in a mesh: rep: 16 (over x, z_lo, core), tp: 8 (over z_hi, y).
Axes of the slice: x: 4, y: 4, z: 4 (z_hi: 2, z_lo: 2; z = z_hi * 2 + z_lo), core: 2. Of those that a mesh axis runs over, the one named last changes fastest.
Arguments:
- flat_buffer: bfloat16 [579207168], P(('rep', 'tp')), may hold values from -60 to 60
- shard_pad: int32 [2, 6], replicated, may hold values from 0 to 2
Outputs:
- q_served: bfloat16 [2, 6144, 6144], P(None, 'rep', 'tp')
- q_scale: float32 [2, 48, 6144], P(None, 'rep', 'tp')
- k_served: bfloat16 [2, 6144, 1024], P(None, 'rep', 'tp')
- k_scale: float32 [2, 48, 1024], P(None, 'rep', 'tp')
- v_served: bfloat16 [2, 6144, 1024], P(None, 'rep', 'tp')
- v_scale: float32 [2, 48, 1024], P(None, 'rep', 'tp')
- o_served: bfloat16 [2, 6144, 6144], P(None, 'tp', 'rep')
- o_scale: float32 [2, 48, 6144], P(None, 'tp', 'rep')
- gate_served: bfloat16 [2, 6144, 16384], P(None, 'rep', 'tp')
- gate_scale: float32 [2, 48, 16384], P(None, 'rep', 'tp')
- up_served: bfloat16 [2, 6144, 16384], P(None, 'rep', 'tp')
- up_scale: float32 [2, 48, 16384], P(None, 'rep', 'tp')
The draws below stay inside these ranges and needn't reach their ends.
All inputs are finite; a program needn't handle non-finite values. Where the reference program divides by a largest or mean magnitude, that divisor is 1e-20 or more.
Results may differ from the reference program's by a relative error of at most 0.001.
Values may be sent and summed in bfloat16 or wider, within the bound.
A program may use at most 128 MiB of HBM per device.

```python
import math
import jax
import jax.numpy as jnp
from jax import lax

D = 6144
KV = 1024
FF = 16384
GROUP = 128
LAYERS = 2
PADMAX = 2
FLAT_DEV = 4525056
FLAT = 579207168
DEVICES = 128


def draw_flat_buffer(key, part):
    first, second = jax.random.split(jax.random.fold_in(key, 17))
    base = jnp.clip(jax.random.normal(first, (FLAT,), jnp.float32), -6.0, 6.0)
    factor = jnp.exp(jax.random.uniform(second, (FLAT // 32,), jnp.float32, 0.0, math.log(10.0)))
    return (base * jnp.repeat(factor, 32)).astype(jnp.bfloat16)


def touch_ends(result, rng, low, high):
    longest = result.shape.index(max(result.shape))
    spots = []
    for shift in (0, 1):
        where = [jax.random.randint(jax.random.fold_in(rng, axis), (), 0, length) for axis, length in enumerate(result.shape)]
        where[longest] = (where[longest] + shift) % result.shape[longest]
        spots.append(tuple(where))
    return result.at[spots[0]].set(low).at[spots[1]].set(high)


def setup_inputs(seed: int = 0) -> dict:
    streams_of = jax.random.split(jax.random.key(seed), 3)
    flat_buffer = draw_flat_buffer(jax.random.fold_in(streams_of[2], 71), 0)
    shard_pad = touch_ends(jax.random.randint(streams_of[1], (LAYERS, 6), 0, PADMAX + 1), jax.random.fold_in(streams_of[1], 1), 0, PADMAX).astype(jnp.int32)
    return {"flat_buffer": flat_buffer, "shard_pad": shard_pad}


def quantize(served):
    values = served.astype(jnp.float32)
    grouped = values.reshape(values.shape[0] // GROUP, GROUP, values.shape[1])
    peak = jnp.max(jnp.abs(grouped), axis=1) + 1e-6
    scaled = (grouped / peak[:, None, :]).astype(jnp.bfloat16)
    return scaled.reshape(served.shape), peak


def reference(flat_buffer, shard_pad):
    widths = (D, KV, KV, D, FF, FF)
    table = flat_buffer.reshape(DEVICES, FLAT_DEV)
    offset = jnp.zeros((), jnp.int32)
    served_all = [[] for index in range(6)]
    scale_all = [[] for index in range(6)]
    for layer in range(LAYERS):
        for index in range(6):
            length = widths[index] // DEVICES * D
            piece = lax.dynamic_slice_in_dim(table, offset.astype(jnp.int32), length, 1)
            whole = piece.reshape(widths[index], D)
            scaled, peak = quantize(whole.T)
            served_all[index].append(scaled)
            scale_all[index].append(peak)
            offset = (offset + length + 128 * shard_pad[layer, index]).astype(jnp.int32)
    outputs = []
    for index in range(6):
        outputs.append(jnp.stack(served_all[index]))
        outputs.append(jnp.stack(scale_all[index]))
    return (outputs[0], outputs[1], outputs[2], outputs[3], outputs[4], outputs[5],
            outputs[6], outputs[7], outputs[8], outputs[9], outputs[10], outputs[11])
```

```python
import functools

import jax
import jax.numpy as jnp
from jax import lax
from jax.experimental import pallas as pl
from jax.experimental.pallas import tpu as pltpu
from jax.sharding import PartitionSpec as P

MESH = pl.DeviceIdType.MESH
BF = jnp.bfloat16
F32 = jnp.float32
CH = 15
ROWS = 35352
LENS = (2304, 384, 384, 2304, 6144, 6144)
BASES = (0, 2304, 2688, 3072, 5376, 11520)
LAYER = 17664
SLACK = 24
Q, K, V, O, GATE, UP = range(6)


def coords():
    r, t = lax.axis_index("rep"), lax.axis_index("tp")
    return r // 4, (r // 2) % 2, r % 2, t // 4, t % 4


def dev(x, y, z, c):
    return ((x * 2 + z % 2) * 2 + c, (z // 2) * 4 + y)


def copy_wait(ref, sem):
    pltpu.make_async_copy(ref, ref, sem).wait()


def offsets(pad_ref):
    out, padding = [], jnp.int32(0)
    for l in range(2):
        for i in range(6):
            out.append(padding + (l * LAYER + BASES[i]))
            padding = padding + pad_ref[l, i]
    return out


def prep_kernel(pad_ref, flat_ref, s_out, o_out, flat, wide, s, o, in_sem, s_sem, o_sem):
    off = offsets(pad_ref)
    order = [(0, GATE), (0, UP), (1, GATE), (1, UP), (0, O), (1, O)]
    order += [(l, i) for l in range(2) for i in (Q, K, V)]

    def region(l, i):
        return l * LAYER + BASES[i], LENS[i] + SLACK

    copies = {}
    for n, (l, i) in enumerate(order):
        start, _ = region(l, i)
        size = LENS[i] + (SLACK if (l, i) == (1, UP) else 0)
        copies[(l, i)] = pltpu.make_async_copy(
            flat_ref.at[pl.ds(start, size)], flat.at[pl.ds(start, size)], in_sem.at[n])
        copies[(l, i)].start()
    for l, i in order:
        copies[(l, i)].wait()

    def widen(n, _):
        rows = pl.ds(pl.multiple_of(n * 128, 128), 128)
        wide[rows] = flat[rows].astype(F32)
        return 0

    lax.fori_loop(0, ROWS // 128, widen, 0)
    tail = pl.ds(ROWS // 128 * 128, ROWS % 128)
    wide[tail] = flat[tail].astype(F32)

    for l in range(2):
        for n, i in enumerate((GATE, UP)):
            for j in range(3):
                k = (l * 2 + n) * 3 + j
                start = off[l * 6 + i] + j

                def block(r, _):
                    rows = wide[pl.ds(start + 3 * r, 128, stride=48)]
                    s[k, r] = rows.T.astype(BF)
                    return 0

                lax.fori_loop(0, 16, block, 0)
                pltpu.make_async_copy(s.at[k], s_out.at[k], s_sem).start()
    for j in range(3):
        k = 12 + j

        def block(r, _):
            for l in range(2):
                c = 3 * r + j
                s[k, r, pl.ds(l * 64, 48)] = wide[pl.ds(off[l * 6 + Q] + c, 48, stride=48)].astype(BF)
                kk = wide[pl.ds(off[l * 6 + K] + c, 8, stride=48)]
                vv = wide[pl.ds(off[l * 6 + V] + c, 8, stride=48)]
                s[k, r, pl.ds(l * 64 + 48, 16)] = jnp.concatenate([kk, vv], axis=0).astype(BF)
            return 0

        lax.fori_loop(0, 16, block, 0)
        pltpu.make_async_copy(s.at[k], s_out.at[k], s_sem).start()

    def oblock(t, _):
        for l in range(2):
            for j in range(6):
                rows = wide[pl.ds(off[l * 6 + O] + 6 * t + j, 48, stride=48)]
                o[t, pl.ds((l * 6 + j) * 48, 48)] = rows.astype(BF)
        return 0

    lax.fori_loop(0, 8, oblock, 0)
    pltpu.make_async_copy(o, o_out, o_sem).start()
    copy_wait(s, s_sem)
    copy_wait(o, o_sem)


def prep(pads, flat):
    return pl.pallas_call(
        prep_kernel,
        out_shape=(jax.ShapeDtypeStruct((CH, 16, 128, 128), BF), jax.ShapeDtypeStruct((8, 576, 128), BF)),
        in_specs=[pl.BlockSpec(memory_space=pltpu.SMEM), pl.BlockSpec(memory_space=pl.ANY)],
        out_specs=[pl.BlockSpec(memory_space=pl.ANY)] * 2,
        scratch_shapes=[
            pltpu.VMEM((ROWS, 128), BF),
            pltpu.VMEM((ROWS, 128), F32),
            pltpu.VMEM((CH, 16, 128, 128), BF),
            pltpu.VMEM((8, 576, 128), BF),
            pltpu.SemaphoreType.DMA((12,)),
            pltpu.SemaphoreType.DMA,
            pltpu.SemaphoreType.DMA,
        ],
        compiler_params=pltpu.CompilerParams(vmem_limit_bytes=60 * 2**20),
    )(pads, flat)


def exchange_kernel(s, o, f, fo, r1, r2, xs, xr, zs, zr, ys, yr, os, orr):
    x, zl, c, zh, y = coords()
    z = zh * 2 + zl
    partners = [dev((x + j) % 4, y, z, c) for j in (1, 2, 3)]
    partners += [dev(x, (y + j) % 4, z, c) for j in (1, 2, 3)]
    partners += [dev(x, y, (z + i // 2) % 4, (c + i % 2) % 2) for i in range(1, 8)]
    partners += [dev(x, (y + i) % 4, (z + 2) % 4, c) for i in range(4)]
    barrier = pltpu.get_barrier_semaphore()
    for d in partners:
        pl.semaphore_signal(barrier, inc=1, device_id=d, device_id_type=MESH)
    pl.semaphore_wait(barrier, len(partners))

    def remote(src, dst, send, recv, d):
        pltpu.make_async_remote_copy(
            src_ref=src, dst_ref=dst, send_sem=send, recv_sem=recv, device_id=d, device_id_type=MESH).start()

    def send_x(k):
        for j in (1, 3, 2):
            xd = (x + j) % 4
            remote(s.at[k, xd], r1.at[k, x], xs, xr.at[k], dev(xd, y, z, c))
        pltpu.make_async_copy(s.at[k, x], r1.at[k, x], xr.at[k]).start()

    def send_z(k):
        for i in (2, 6, 4, 3, 7, 5, 1):
            zd, cd = (z + i // 2) % 4, (c + i % 2) % 2
            remote(r1.at[k, pl.ds(zd // 2 * 2, 2), zd % 2, cd], r2.at[k, :, zl, zh, c], zs, zr.at[k], dev(x, y, zd, cd))
        pltpu.make_async_copy(r1.at[k, pl.ds(zh * 2, 2), zl, c], r2.at[k, :, zl, zh, c], zr.at[k]).start()

    def send_y(k):
        for j in (1, 3, 2):
            yd = (y + j) % 4
            remote(r2.at[k, yd // 2, yd % 2], f.at[k, y], ys, yr, dev(x, yd, z, c))
        pltpu.make_async_copy(r2.at[k, y // 2, y % 2], f.at[k, y], yr).start()

    for i in (1, 3, 2, 5, 7, 6, 4):
        yd, zhd = (y + i % 4) % 4, (zh + i // 4) % 2
        remote(o.at[zhd * 4 + yd], fo.at[zh * 4 + y], os, orr, dev(x, yd, zhd * 2 + zl, c))
    pltpu.make_async_copy(o.at[zh * 4 + y], fo.at[zh * 4 + y], orr).start()

    def first(k, _):
        send_x(k)
        return 0

    lax.fori_loop(0, CH, first, 0)

    def step(k, _):
        copy_wait(r1.at[k], xr.at[k])
        send_z(k)

        @pl.when(k > 0)
        def _():
            copy_wait(r2.at[k - 1], zr.at[k - 1])
            send_y(k - 1)

        return 0

    lax.fori_loop(0, CH, step, 0)
    copy_wait(r2.at[CH - 1], zr.at[CH - 1])
    send_y(CH - 1)
    copy_wait(f, yr)
    copy_wait(fo, orr)
    copy_wait(s.at[:, pl.ds(0, 3)], xs)
    copy_wait(s.at[:, pl.ds(0, 3)], ys)
    copy_wait(s.at[:, pl.ds(0, 3)], zs)
    copy_wait(s.at[:, 0, 0], zs)
    copy_wait(fo.at[pl.ds(0, 7)], os)


def exchange(s, o):
    dma = pltpu.SemaphoreType.DMA
    return pl.pallas_call(
        exchange_kernel,
        out_shape=(jax.ShapeDtypeStruct((CH, 4, 2, 2, 128, 128), BF), jax.ShapeDtypeStruct((8, 576, 128), BF)),
        in_specs=[pl.BlockSpec(memory_space=pl.ANY)] * 2,
        out_specs=[pl.BlockSpec(memory_space=pl.ANY)] * 2,
        scratch_shapes=[
            pltpu.VMEM((CH, 4, 2, 2, 128, 128), BF),
            pltpu.VMEM((CH, 2, 2, 2, 2, 128, 128), BF),
            dma, dma((CH,)), dma, dma((CH,)), dma, dma, dma, dma,
        ],
        compiler_params=pltpu.CompilerParams(
            collective_id=0, has_side_effects=True, vmem_limit_bytes=60 * 2**20),
    )(s, o)


def quantize(values):
    peak = jnp.max(jnp.abs(values), axis=0, keepdims=True) + 1e-6
    return (values * (1.0 / peak)).astype(BF), peak


def finish_kernel(f_ref, fo_ref, q, qs, k, ks, v, vs, o, os, gate, gs, up, us,
                  f, fo, qb, kb, vb, ob, gb, in_sem, o_sem, out_sem):
    for n in range(CH):
        pltpu.make_async_copy(f_ref.at[n], f.at[n], in_sem.at[n]).start()
    pltpu.make_async_copy(fo_ref, fo, o_sem).start()

    def put(src, dst, n):
        pltpu.make_async_copy(src, dst, out_sem.at[n]).start()

    for n in range(12):
        copy_wait(f.at[n], in_sem.at[n])
        l, which, j = n // 6, n // 3 % 2, n % 3
        scale = (gs, us)[which]
        for src in range(16):
            c, zh, y = src // 8, src // 4 % 2, src % 4
            cols = pl.ds(src * 128, 128)
            scaled, peak = quantize(f[n, y, zh, c].astype(F32))
            gb[n, :, cols] = scaled
            scale[j, pl.ds(l, 1), cols] = peak
        put(gb.at[n], (gate, up)[which].at[l, pl.ds(j * 128, 128)], 0)
    sources = [(s % 4, s // 4 % 2, s // 8) for s in range(16)]
    for j in range(3):
        n = 12 + j
        copy_wait(f.at[n], in_sem.at[n])
        for l in range(2):
            base = l * 64
            rows = [f[n, y, zh, c, pl.ds(base, 48)].astype(F32) for y, zh, c in sources]
            qb[l, j], qs[j, pl.ds(l, 1)] = quantize(jnp.concatenate(rows, axis=0).T)
            both = [f[n, y, zh, c, pl.ds(base + 48, 16)].astype(F32) for y, zh, c in sources]
            kb[l, j], ks[j, pl.ds(l, 1)] = quantize(jnp.concatenate([b[:8] for b in both], axis=0).T)
            vb[l, j], vs[j, pl.ds(l, 1)] = quantize(jnp.concatenate([b[8:] for b in both], axis=0).T)
            rows = pl.ds(j * 128, 128)
            put(qb.at[l, j], q.at[l, rows], 1)
            put(kb.at[l, j], k.at[l, rows], 2)
            put(vb.at[l, j], v.at[l, rows], 3)
    copy_wait(fo, o_sem)
    for l in range(2):
        for j in range(6):
            rows = [fo[t, pl.ds((l * 6 + j) * 48, 48)].astype(F32) for t in range(8)]
            ob[l, j], os[j, pl.ds(l, 1)] = quantize(jnp.concatenate(rows, axis=0).T)
            put(ob.at[l, j], o.at[l, pl.ds(j * 128, 128)], 4)
    for n, buffer in enumerate((gb, qb, kb, vb, ob)):
        copy_wait(buffer, out_sem.at[n])


def finish(f, fo):
    shapes = [((2, 384, 768), (3, 2, 768)), ((2, 384, 128), (3, 2, 128)), ((2, 384, 128), (3, 2, 128)),
              ((2, 768, 384), (6, 2, 384)), ((2, 384, 2048), (3, 2, 2048)), ((2, 384, 2048), (3, 2, 2048))]
    out_shape, out_specs = [], []
    for served, scale in shapes:
        out_shape += [jax.ShapeDtypeStruct(served, BF), jax.ShapeDtypeStruct(scale, F32)]
        out_specs += [pl.BlockSpec(memory_space=pl.ANY), pl.BlockSpec(memory_space=pltpu.VMEM)]
    dma = pltpu.SemaphoreType.DMA
    return pl.pallas_call(
        finish_kernel,
        out_shape=out_shape,
        in_specs=[pl.BlockSpec(memory_space=pl.ANY)] * 2,
        out_specs=out_specs,
        scratch_shapes=[
            pltpu.VMEM((CH, 4, 2, 2, 128, 128), BF),
            pltpu.VMEM((8, 576, 128), BF),
            pltpu.VMEM((2, 3, 128, 768), BF),
            pltpu.VMEM((2, 3, 128, 128), BF),
            pltpu.VMEM((2, 3, 128, 128), BF),
            pltpu.VMEM((2, 6, 128, 384), BF),
            pltpu.VMEM((12, 128, 2048), BF),
            dma((CH,)), dma, dma((5,)),
        ],
        compiler_params=pltpu.CompilerParams(vmem_limit_bytes=60 * 2**20),
    )(f, fo)


def local(flat, pads):
    s, o = prep(pads, flat.reshape(ROWS, 128))
    f, fo = exchange(s.reshape(CH, 4, 2, 2, 128, 128), o)
    outs = finish(f, fo)
    return tuple(a.transpose(1, 0, 2) if n % 2 else a for n, a in enumerate(outs))


def solution(mesh):
    a, b = P(None, "rep", "tp"), P(None, "tp", "rep")
    specs = (a, a, a, a, a, a, b, b, a, a, a, a)
    return jax.shard_map(
        local, mesh=mesh, in_specs=(P(("rep", "tp")), P()), out_specs=specs, check_vma=False)
```
